128 devices in a mesh: jown: 8 (over y, core), pown: 16 (over x, z).
Axes of the slice: x: 4, y: 4, z: 4, core: 2. Of those that a mesh axis runs over, the one named last changes fastest.
Arguments:
- vertex: bfloat16 [128, 1024, 1024], P(('jown', 'pown')), may hold values from -6 to 6
- bare: bfloat16 [128, 1024, 1024], P(('jown', 'pown')), may hold values from -0.1875 to 0.1875
- pp_prop: float32 [128, 1024], P(('jown', 'pown')), may hold values from 0.3 to 3
- ph_prop: float32 [128, 1024], P(('jown', 'pown')), may hold values from 0.3 to 3
- orders: int32 [128], replicated, may hold values from 512 to 1024, as said below
- pandya_src: int32 [128, 4], replicated, may hold values from 0 to 127
- pandya_sixj: float32 [128, 4, 1024], P(None, None, ('jown', 'pown')), may hold values from -1 to 1
- back_src: int32 [128, 4], replicated, may hold values from 0 to 127
- back_sixj: float32 [128, 4, 1024], P(None, None, ('jown', 'pown')), may hold values from -1 to 1
Outputs:
- updated: bfloat16 [128, 1024, 1024], P(('jown', 'pown'))
The draws below stay inside these ranges and needn't reach their ends.
Inputs may be any that keep to these rules, and one draw needn't show every extreme that they name: `orders`: some block has order exactly 1024.
All inputs are finite; a program needn't handle non-finite values.
Results may differ from the reference program's by a relative error of at most 0.0055.
Values may be sent and summed in bfloat16 or wider, within the bound.
A program may use at most 64 MiB of HBM per device.

```python
import math
import jax
import jax.numpy as jnp
from jax import lax

M = 1024
TERMS = 4
BLOCKS = 128


def draw_orders(key, part):
    first_key, second_key = jax.random.split(jax.random.fold_in(key, 17))
    base = jax.random.randint(first_key, (BLOCKS,), M // 2, M + 1)
    chosen = jax.random.randint(second_key, (), 0, BLOCKS)
    return base.at[chosen].set(M).astype(jnp.int32)


def with_ends(drawn, key, least, largest):
    shape = drawn.shape
    place = [jax.random.randint(jax.random.fold_in(key, axis), (), 0, shape[axis]) for axis in range(len(shape))]
    drawn = drawn.at[tuple(place)].set(least)
    longest = shape.index(max(shape))
    place[longest] = (place[longest] + 1) % shape[longest]
    return drawn.at[tuple(place)].set(largest)


def steps_of(rng, shape, cuts, smallest, high):
    gain, own = 1.0, jax.random.fold_in(rng, 6)
    for position, blocks in cuts:
        steps = jnp.exp(jax.random.uniform(jax.random.fold_in(own, position), (blocks,), jnp.float32, smallest / len(cuts), high / len(cuts)))
        gain = gain * jnp.repeat(steps, shape[position] // blocks).reshape([-1 if axis == position else 1 for axis in range(len(shape))])
    return gain


def bell_draw(own_key, extent, spread, limit, shards=(), dtype=jnp.bfloat16):
    level = steps_of(own_key, extent, shards, -0.22, 0.18) if shards else 1.0
    values = jax.random.normal(own_key, extent, jnp.float32) * spread * level
    return jnp.minimum(jnp.maximum(values, -limit), limit).astype(dtype)


def setup_inputs(seed: int = 0) -> dict:
    streams_of = jax.random.split(jax.random.key(seed), 10)
    return {
        "vertex": bell_draw(streams_of[0], (BLOCKS, M, M), 1.0, 6.0, ((0, 128),)),
        "bare": bell_draw(streams_of[1], (BLOCKS, M, M), M ** -0.5, 0.1875, ((0, 128),)),
        "pp_prop": jnp.clip(jnp.exp(math.log(3.0) - 2.3025851 * jax.random.uniform(streams_of[2], (BLOCKS, M), jnp.float32) ** steps_of(streams_of[2], (BLOCKS, M), ((0, 128),), -0.2, 0.2)), 0.3, 3.0),
        "ph_prop": jnp.clip(jnp.exp(math.log(3.0) - 2.3025851 * jax.random.uniform(streams_of[3], (BLOCKS, M), jnp.float32) ** steps_of(streams_of[3], (BLOCKS, M), ((0, 128),), -0.2, 0.2)), 0.3, 3.0),
        "orders": draw_orders(jax.random.fold_in(streams_of[9], 71), 0),
        "pandya_src": with_ends(jax.random.randint(streams_of[5], (BLOCKS, TERMS), 0, BLOCKS), jax.random.fold_in(streams_of[5], 1), 0, BLOCKS - 1).astype(jnp.int32),
        "pandya_sixj": jnp.clip(jax.random.uniform(streams_of[6], (BLOCKS, TERMS, M), jnp.float32, -1.0, 1.0) * steps_of(streams_of[6], (BLOCKS, TERMS, M), ((2, 128),), -0.4, 0.0), -1.0, 1.0),
        "back_src": with_ends(jax.random.randint(streams_of[7], (BLOCKS, TERMS), 0, BLOCKS), jax.random.fold_in(streams_of[7], 1), 0, BLOCKS - 1).astype(jnp.int32),
        "back_sixj": jnp.clip(jax.random.uniform(streams_of[8], (BLOCKS, TERMS, M), jnp.float32, -1.0, 1.0) * steps_of(streams_of[8], (BLOCKS, TERMS, M), ((2, 128),), -0.4, 0.0), -1.0, 1.0),
    }


def pair_mask(order):
    live = (jnp.arange(M) < order).astype(jnp.float32)
    return live[:, None] * live[None, :]

def recouple(blocks, sources, factors, orders):

    def single(item):
        picks, weights, order = item
        summed = jnp.zeros((M, M), jnp.float32)
        for term in range(picks.shape[0]):
            summed = summed + weights[term][:, None] * blocks[picks[term]].astype(jnp.float32)
        return (summed * pair_mask(order)).astype(jnp.bfloat16)
    return lax.map(single, (sources, factors, orders))

def reference(vertex, bare, pp_prop, ph_prop, orders, pandya_src, pandya_sixj, back_src, back_sixj):

    def mask_one(item):
        block, order = item
        return (block.astype(jnp.float32) * pair_mask(order)).astype(jnp.bfloat16)
    masked = lax.map(mask_one, (vertex, orders))
    ph = recouple(masked, pandya_src, pandya_sixj, orders)

    def cycle_one(item):
        block, prop = item
        weighted = (block.astype(jnp.float32) * prop[None, :]).astype(jnp.bfloat16)
        product = jnp.dot(weighted, block, preferred_element_type=jnp.float32)
        return (product * (1.0 / math.sqrt(M))).astype(jnp.bfloat16)
    cycle = lax.map(cycle_one, (ph, ph_prop))
    returned = recouple(cycle, back_src, back_sixj, orders)

    def final_one(item):
        block, interaction, prop, back, order = item
        scaled = (prop[:, None] * block.astype(jnp.float32)).astype(jnp.bfloat16)
        ladder = jnp.dot(interaction, scaled, preferred_element_type=jnp.float32)
        total = block.astype(jnp.float32) + ladder + back.astype(jnp.float32)
        return (total * pair_mask(order)).astype(jnp.bfloat16)
    return lax.map(final_one, (masked, bare, pp_prop, returned, orders))
```

```python
import functools
import math

import jax
import jax.numpy as jnp
from jax import lax
from jax.experimental import pallas as pl
from jax.experimental.pallas import tpu as pltpu
from jax.sharding import PartitionSpec as P

MESH = pl.DeviceIdType.MESH
F32, BF16 = jnp.float32, jnp.bfloat16
STRIDE = 37


def kernel(
    dims,
    orders_ref,
    psrc_ref,
    bsrc_ref,
    bands_ref,
    vertex_ref,
    bare_ref,
    pp_ref,
    php_ref,
    psix_ref,
    bsix_ref,
    out_ref,
    vbuf,
    bbuf,
    base,
    wide,
    recv_a,
    mix_a,
    ph_bands,
    ph,
    weighted,
    cyc,
    recv_b,
    mix_b,
    ret_bands,
    load_sem,
    send_sem,
    recv_sem,
):
    n_j, n_p, n_y, n_x, n_z, cores = dims
    total = n_j * n_p
    m = ph.shape[0]
    band = m // total
    tiles = m // 128
    me_j, me_p = lax.axis_index("jown"), lax.axis_index("pown")
    me = me_j * n_p + me_p
    my_y, my_c = me_j // cores, me_j % cores
    my_x, my_z = me_p // n_z, me_p % n_z

    def peer_of(step):
        o = (step * STRIDE) % total
        z = (my_z + o % n_z) % n_z
        o = o // n_z
        x = (my_x + o % n_x) % n_x
        o = o // n_x
        c = (my_c + o % cores) % cores
        o = o // cores
        y = (my_y + o) % n_y
        return y * cores + c, x * n_z + z

    def exchange(src, dst, phase):
        @pl.loop(1, total)
        def _(step):
            j, p = peer_of(step)
            pltpu.make_async_remote_copy(
                src_ref=src.at[j * n_p + p],
                dst_ref=dst.at[me],
                send_sem=send_sem.at[phase],
                recv_sem=recv_sem.at[phase],
                device_id=(j, p),
                device_id_type=MESH,
            ).start()

    def arrived(dst, phase):
        part = dst.at[pl.ds(0, total - 1)]
        pltpu.make_async_copy(part, part, recv_sem.at[phase]).wait()

    def sent(src, phase):
        part = src.at[pl.ds(0, total - 1)]
        pltpu.make_async_copy(part, part, send_sem.at[phase]).wait()

    own = pltpu.make_async_copy(bands_ref.at[me], recv_a.at[me], load_sem.at[0])
    own.start()
    load_v = pltpu.make_async_copy(vertex_ref, vbuf, load_sem.at[1])
    load_v.start()
    load_b = pltpu.make_async_copy(bare_ref, bbuf, load_sem.at[2])
    load_b.start()
    exchange(bands_ref, recv_a, 0)

    my_order = orders_ref[me]
    sub = lax.broadcasted_iota(jnp.int32, (8, 128), 0)
    lane = lax.broadcasted_iota(jnp.int32, (8, 128), 1)
    row_id = me * band + sub

    def spread(six_ref, slot):
        for k in range(4):
            six = six_ref[k]
            for c in range(total):
                wide[slot, c, k] = jnp.broadcast_to(six[:, c : c + 1], (8, 128))

    spread(psix_ref, 0)
    spread(bsix_ref, 1)

    load_v.wait()
    load_b.wait()
    col_live = (lax.broadcasted_iota(jnp.int32, (1, m), 1) < my_order).astype(F32)

    @pl.loop(0, m // 128)
    def _(i):
        rows = pl.ds(pl.multiple_of(i * 128, 128), 128)
        ids = i * 128 + lax.broadcasted_iota(jnp.int32, (128, 1), 0)
        row_live = (ids < my_order).astype(F32)
        masked = vbuf[rows, :].astype(F32) * col_live * row_live
        base[rows, :] = masked
        weighted[rows, :] = (masked * pp_ref[rows, :]).astype(BF16)

    @pl.loop(0, m // 128)
    def _(i):
        rows = pl.ds(pl.multiple_of(i * 128, 128), 128)
        base[rows, :] += jnp.dot(bbuf[rows, :], weighted[...], preferred_element_type=F32)

    def recouple(recv, mix, src_ref, slot, source_mask):
        @pl.loop(0, total)
        def _(c):
            order = orders_ref[c]
            acc = [jnp.zeros((8, 128), F32) for _ in range(tiles)]
            for k in range(4):
                s = src_ref[k, c]
                bound = order
                if source_mask:
                    bound = jnp.minimum(order, orders_ref[s])
                w = jnp.where(row_id < bound, wide[slot, c, k], 0.0)
                x = recv[s].astype(F32)
                for t in range(tiles):
                    term = w * x[8 * t : 8 * t + 8]
                    if source_mask:
                        term = jnp.where(lane + 128 * t < bound, term, 0.0)
                    acc[t] = acc[t] + term
            if not source_mask:
                acc = [jnp.where(lane + 128 * t < order, a, 0.0) for t, a in enumerate(acc)]
            mix[c] = jnp.concatenate(acc, axis=0).astype(BF16)

    arrived(recv_a, 0)
    own.wait()
    recouple(recv_a, mix_a, psrc_ref, 0, True)
    exchange(mix_a, ph_bands, 1)
    ph_bands[me] = mix_a[me]
    arrived(ph_bands, 1)

    @pl.loop(0, total // 2)
    def _(q):
        a = ph_bands[2 * q].astype(F32)
        b = ph_bands[2 * q + 1].astype(F32)
        rows = pl.ds(pl.multiple_of(q * 16, 16), 16)
        for t in range(tiles):
            cols = slice(128 * t, 128 * t + 128)
            tile = jnp.concatenate([a[8 * t : 8 * t + 8], b[8 * t : 8 * t + 8]], axis=0)
            ph[rows, cols] = tile.astype(BF16)
            weighted[rows, cols] = (tile * php_ref[:, cols]).astype(BF16)

    @pl.loop(0, m // 128)
    def _(i):
        rows = pl.ds(pl.multiple_of(i * 128, 128), 128)
        prod = jnp.dot(weighted[rows, :], ph[...], preferred_element_type=F32) * (1.0 / math.sqrt(m))
        for b in range(128 // band):
            parts = [prod[band * b : band * b + band, 128 * t : 128 * t + 128] for t in range(tiles)]
            cyc[i * (128 // band) + b] = jnp.concatenate(parts, axis=0).astype(BF16)

    exchange(cyc, recv_b, 2)
    recv_b[me] = cyc[me]
    arrived(recv_b, 2)
    recouple(recv_b, mix_b, bsrc_ref, 1, False)
    exchange(mix_b, ret_bands, 3)
    ret_bands[me] = mix_b[me]
    arrived(ret_bands, 3)

    @pl.loop(0, total // 2)
    def _(q):
        a = ret_bands[2 * q].astype(F32)
        b = ret_bands[2 * q + 1].astype(F32)
        rows = pl.ds(pl.multiple_of(q * 16, 16), 16)
        ids = q * 16 + lax.broadcasted_iota(jnp.int32, (16, 128), 0)
        for t in range(tiles):
            cols = slice(128 * t, 128 * t + 128)
            tile = jnp.concatenate([a[8 * t : 8 * t + 8], b[8 * t : 8 * t + 8]], axis=0)
            col_ids = 128 * t + lax.broadcasted_iota(jnp.int32, (16, 128), 1)
            keep = (ids < my_order) & (col_ids < my_order)
            out_ref[rows, cols] = jnp.where(keep, base[rows, cols] + tile, 0.0).astype(BF16)

    sent(recv_a, 0)
    sent(mix_a, 1)
    sent(cyc, 2)
    sent(mix_b, 3)


def per_device(dims, vertex, bare, pp_prop, ph_prop, orders, pandya_src, pandya_sixj, back_src, back_sixj):
    m = vertex.shape[1]
    n_j, n_p = dims[:2]
    total = n_j * n_p
    band = m // total
    tiles = m // 128
    flat = vertex.reshape(m, m)
    bands = flat.reshape(total, band, tiles, 128).transpose(0, 2, 1, 3).reshape(total, tiles * band, 128)
    tile_buf = pltpu.VMEM((total, tiles * band, 128), BF16)
    square = pltpu.VMEM((m, m), BF16)
    smem = pl.BlockSpec(memory_space=pltpu.SMEM)
    vmem = pl.BlockSpec(memory_space=pltpu.VMEM)
    hbm = pl.BlockSpec(memory_space=pl.ANY)
    out = pl.pallas_call(
        functools.partial(kernel, dims),
        out_shape=jax.ShapeDtypeStruct((m, m), BF16),
        in_specs=[smem] * 3 + [hbm] * 3 + [vmem] * 4,
        out_specs=vmem,
        scratch_shapes=[
            square,
            square,
            pltpu.VMEM((m, m), F32),
            pltpu.VMEM((2, total, 4, 8, 128), F32),
            tile_buf,
            tile_buf,
            tile_buf,
            square,
            square,
            tile_buf,
            tile_buf,
            tile_buf,
            tile_buf,
            pltpu.SemaphoreType.DMA((3,)),
            pltpu.SemaphoreType.DMA((4,)),
            pltpu.SemaphoreType.DMA((4,)),
        ],
        compiler_params=pltpu.CompilerParams(has_side_effects=True, vmem_limit_bytes=56 * 1024 * 1024),
        name="parquet",
    )(
        orders,
        pandya_src.T,
        back_src.T,
        bands,
        flat,
        bare.reshape(m, m),
        pp_prop.reshape(m, 1),
        ph_prop,
        pandya_sixj.transpose(1, 2, 0),
        back_sixj.transpose(1, 2, 0),
    )
    return out.reshape(1, m, m)


def solution(mesh):
    n_j, n_p = mesh.shape["jown"], mesh.shape["pown"]
    cores = 2
    side = math.isqrt(n_p)
    dims = (n_j, n_p, n_j // cores, side, n_p // side, cores)
    placed = (
        P(("jown", "pown"), None, None),
        P(("jown", "pown"), None, None),
        P(("jown", "pown"), None),
        P(("jown", "pown"), None),
        P(),
        P(),
        P(None, None, ("jown", "pown")),
        P(),
        P(None, None, ("jown", "pown")),
    )
    return jax.shard_map(
        functools.partial(per_device, dims),
        mesh=mesh,
        in_specs=placed,
        out_specs=P(("jown", "pown"), None, None),
        check_vma=False,
    )
```

```python
import functools
import math

import jax
import jax.numpy as jnp
from jax import lax
from jax.experimental import pallas as pl
from jax.experimental.pallas import tpu as pltpu
from jax.sharding import PartitionSpec as P

MESH = pl.DeviceIdType.MESH
F32, BF16 = jnp.float32, jnp.bfloat16
STRIDE = 37
PARTS = 2
VMEM_MIB = 42


def kernel(
    dims,
    orders_hbm,
    psrc_hbm,
    bsrc_hbm,
    bands_hbm,
    vertex_hbm,
    bare_hbm,
    pp_hbm,
    php_hbm,
    psix_hbm,
    bsix_hbm,
    out_ref,
    orders_ref,
    psrc_ref,
    bsrc_ref,
    pp_ref,
    php_ref,
    psix_ref,
    bsix_ref,
    vbuf,
    bbuf,
    base,
    wide,
    mix_a,
    ph_bands,
    ph,
    weighted,
    cyc,
    mix_b,
    ret_bands,
    load_sem,
    send_sem,
    recv_sem,
    gate_sem,
    *recv,
):
    recv_a, recv_b = recv[:PARTS], recv[PARTS:]
    n_j, n_p, n_y, n_x, n_z, cores = dims
    total = n_j * n_p
    m = ph.shape[0]
    band = m // total
    tiles = m // 128 // PARTS
    me_j, me_p = lax.axis_index("jown"), lax.axis_index("pown")
    me = me_j * n_p + me_p
    my_y, my_c = me_j // cores, me_j % cores
    my_x, my_z = me_p // n_z, me_p % n_z

    def shifted(y, c, x, z):
        j = (my_y + y) % n_y * cores + (my_c + c) % cores
        return j, (my_x + x) % n_x * n_z + (my_z + z) % n_z

    def peer_of(step):
        o = (step * STRIDE) % total
        z = o % n_z
        o = o // n_z
        x = o % n_x
        o = o // n_x
        return shifted(o // cores, o % cores, x, z)

    def send(src, dst, phase, part, j, p):
        pltpu.make_async_remote_copy(
            src_ref=src,
            dst_ref=dst,
            send_sem=send_sem.at[phase],
            recv_sem=recv_sem.at[phase, part],
            device_id=(j, p),
            device_id_type=MESH,
        ).start()

    def arrived(phase, part):
        span = mix_a.at[0, pl.ds(0, total - 1)]
        pltpu.make_async_copy(span, span, recv_sem.at[phase, part]).wait()

    barrier = pltpu.get_barrier_semaphore()
    column = [(o // cores, o % cores, 0, 0) for o in range(1, n_j)]
    plane = [(0, 0, o // n_z, o % n_z) for o in range(1, n_p)]
    for offset in column + plane:
        pl.semaphore_signal(barrier, inc=1, device_id=shifted(*offset), device_id_type=MESH)

    def load(src, dst, slot):
        copy = pltpu.make_async_copy(src, dst, load_sem.at[slot])
        copy.start()
        return copy

    rows_of = [pl.ds(part * tiles * band, tiles * band) for part in range(PARTS)]
    own = [load(bands_hbm.at[me, rows_of[part]], recv_a[part].at[me], 9 + part) for part in range(PARTS)]
    loads = [
        load(src, dst, slot)
        for slot, (src, dst) in enumerate(
            (
                (orders_hbm, orders_ref),
                (psrc_hbm, psrc_ref),
                (bsrc_hbm, bsrc_ref),
                (pp_hbm, pp_ref),
                (php_hbm, php_ref),
                (psix_hbm, psix_ref),
                (bsix_hbm, bsix_ref),
                (vertex_hbm, vbuf),
                (bare_hbm, bbuf),
            )
        )
    ]
    pl.semaphore_wait(barrier, len(column) + len(plane))
    for offset in column:
        pl.semaphore_signal(gate_sem, inc=1, device_id=shifted(*offset), device_id_type=MESH)
    pl.semaphore_wait(gate_sem, len(column))

    for part in range(PARTS):

        @pl.loop(1, total)
        def _(step):
            j, p = peer_of(step)
            send(bands_hbm.at[j * n_p + p, rows_of[part]], recv_a[part].at[me], 0, part, j, p)

    for copy in loads:
        copy.wait()
    my_order = orders_ref[me]
    lane = lax.broadcasted_iota(jnp.int32, (8, 128), 1)
    row_id = me * band + lax.broadcasted_iota(jnp.int32, (8, 128), 0)

    def spread(six_ref, slot):
        for k in range(4):
            six = six_ref[k]
            for c in range(total):
                wide[slot, c, k] = jnp.broadcast_to(six[:, c : c + 1], (8, 128))

    spread(psix_ref, 0)

    col_live = (lax.broadcasted_iota(jnp.int32, (1, m), 1) < my_order).astype(F32)

    @pl.loop(0, m // 128)
    def _(i):
        rows = pl.ds(pl.multiple_of(i * 128, 128), 128)
        ids = i * 128 + lax.broadcasted_iota(jnp.int32, (128, 1), 0)
        row_live = (ids < my_order).astype(F32)
        scale = jnp.broadcast_to(pp_ref[:, rows], (128, 128)).T
        masked = vbuf[rows, :].astype(F32) * col_live * row_live
        base[rows, :] = masked
        for t in range(m // 128):
            cols = slice(128 * t, 128 * t + 128)
            weighted[rows, cols] = (masked[:, cols] * scale).astype(BF16)

    @pl.loop(0, m // 256)
    def _(i):
        rows = pl.ds(pl.multiple_of(i * 256, 256), 256)
        base[rows, :] += jnp.dot(bbuf[rows, :], weighted[...], preferred_element_type=F32)

    spread(bsix_ref, 1)

    def recouple(recv, part, mix, landing, src_ref, slot, source_mask, phase):
        first = 128 * tiles * part

        def mixed(c):
            order = orders_ref[c]
            acc = [jnp.zeros((8, 128), F32) for _ in range(tiles)]
            for k in range(4):
                s = src_ref[k, c]
                bound = order
                if source_mask:
                    bound = jnp.minimum(order, orders_ref[s])
                w = jnp.where(row_id < bound, wide[slot, c, k], 0.0)
                x = recv[s].astype(F32)
                for t in range(tiles):
                    term = w * x[8 * t : 8 * t + 8]
                    if source_mask:
                        term = jnp.where(lane + (first + 128 * t) < bound, term, 0.0)
                    acc[t] = acc[t] + term
            if not source_mask:
                acc = [jnp.where(lane + (first + 128 * t) < order, a, 0.0) for t, a in enumerate(acc)]
            return jnp.concatenate(acc, axis=0).astype(BF16)

        def store(step):
            j, p = peer_of(step)
            c = j * n_p + p
            mix[part, c] = mixed(c)

        def leave(step):
            j, p = peer_of(step)
            send(mix.at[part, j * n_p + p], landing.at[part, me], phase, part, j, p)

        store(1)

        @pl.loop(2, total)
        def _(step):
            store(step)
            leave(step - 1)

        landing[part, me] = mixed(me)
        leave(total - 1)

    for part in range(PARTS):
        own[part].wait()
        arrived(0, part)
        recouple(recv_a[part], part, mix_a, ph_bands, psrc_ref, 0, True, 1)

    def pair(bands, part, q):
        a = bands[part, 2 * q].astype(F32)
        b = bands[part, 2 * q + 1].astype(F32)
        return [
            jnp.concatenate([a[8 * t : 8 * t + 8], b[8 * t : 8 * t + 8]], axis=0) for t in range(tiles)
        ]

    for part in range(PARTS):
        arrived(1, part)

        @pl.loop(0, total // 2)
        def _(q):
            rows = pl.ds(pl.multiple_of(q * 16, 16), 16)
            for t, tile in enumerate(pair(ph_bands, part, q)):
                first = 128 * (part * tiles + t)
                cols = slice(first, first + 128)
                ph[rows, cols] = tile.astype(BF16)
                weighted[rows, cols] = (tile * php_ref[:, cols]).astype(BF16)

    for part in range(PARTS):
        cols = slice(128 * tiles * part, 128 * tiles * (part + 1))

        @pl.loop(0, m // 256)
        def _(i):
            rows = pl.ds(pl.multiple_of(i * 256, 256), 256)
            prod = jnp.dot(weighted[rows, :], ph[:, cols], preferred_element_type=F32)
            prod = prod * (1.0 / math.sqrt(m))
            for b in range(256 // band):
                lines = [prod[band * b : band * b + band, 128 * t : 128 * t + 128] for t in range(tiles)]
                cyc[part, i * (256 // band) + b] = jnp.concatenate(lines, axis=0).astype(BF16)

        @pl.loop(1, total)
        def _(step):
            j, p = peer_of(step)
            send(cyc.at[part, j * n_p + p], recv_b[part].at[me], 2, part, j, p)

        recv_b[part][me] = cyc[part, me]

    for part in range(PARTS):
        arrived(2, part)
        recouple(recv_b[part], part, mix_b, ret_bands, bsrc_ref, 1, False, 3)

    for part in range(PARTS):
        arrived(3, part)

        @pl.loop(0, total // 2)
        def _(q):
            rows = pl.ds(pl.multiple_of(q * 16, 16), 16)
            ids = q * 16 + lax.broadcasted_iota(jnp.int32, (16, 128), 0)
            for t, tile in enumerate(pair(ret_bands, part, q)):
                first = 128 * (part * tiles + t)
                cols = slice(first, first + 128)
                col_ids = first + lax.broadcasted_iota(jnp.int32, (16, 128), 1)
                keep = (ids < my_order) & (col_ids < my_order)
                out_ref[rows, cols] = jnp.where(keep, base[rows, cols] + tile, 0.0).astype(BF16)

    for phase in range(4):
        span = mix_a.at[:, pl.ds(0, total - 1)]
        pltpu.make_async_copy(span, span, send_sem.at[phase]).wait()


def per_device(dims, vertex, bare, pp_prop, ph_prop, orders, pandya_src, pandya_sixj, back_src, back_sixj):
    m = vertex.shape[1]
    n_j, n_p = dims[:2]
    total = n_j * n_p
    band = m // total
    tiles = m // 128
    flat = vertex.reshape(m, m)
    bands = flat.reshape(total, band, tiles, 128).transpose(0, 2, 1, 3).reshape(total, tiles * band, 128)
    tile_buf = pltpu.VMEM((PARTS, total, tiles * band // PARTS, 128), BF16)
    part_buf = pltpu.VMEM((total, tiles * band // PARTS, 128), BF16)
    square = pltpu.VMEM((m, m), BF16)
    vmem = pl.BlockSpec(memory_space=pltpu.VMEM)
    hbm = pl.BlockSpec(memory_space=pltpu.HBM)
    out = pl.pallas_call(
        functools.partial(kernel, dims),
        out_shape=jax.ShapeDtypeStruct((m, m), BF16),
        in_specs=[hbm] * 10,
        out_specs=vmem,
        scratch_shapes=[
            pltpu.SMEM((total,), jnp.int32),
            pltpu.SMEM((4, total), jnp.int32),
            pltpu.SMEM((4, total), jnp.int32),
            pltpu.VMEM((1, m), F32),
            pltpu.VMEM((1, m), F32),
            pltpu.VMEM((4, band, total), F32),
            pltpu.VMEM((4, band, total), F32),
            square,
            square,
            pltpu.VMEM((m, m), F32),
            pltpu.VMEM((2, total, 4, 8, 128), F32),
            tile_buf,
            tile_buf,
            square,
            square,
            tile_buf,
            tile_buf,
            tile_buf,
            pltpu.SemaphoreType.DMA((9 + PARTS,)),
            pltpu.SemaphoreType.DMA((4,)),
            pltpu.SemaphoreType.DMA((4, PARTS)),
            pltpu.SemaphoreType.REGULAR,
        ]
        + [part_buf] * (2 * PARTS),
        compiler_params=pltpu.CompilerParams(collective_id=0, has_side_effects=True, vmem_limit_bytes=VMEM_MIB * 1024 * 1024),
        name="parquet",
    )(
        *(pltpu.with_memory_space_constraint(a, pltpu.HBM) for a in (
        orders,
        pandya_src.T,
        back_src.T,
        bands,
        flat,
        bare.reshape(m, m),
        pp_prop,
        ph_prop,
        pandya_sixj.transpose(1, 2, 0),
        back_sixj.transpose(1, 2, 0),
    )))
    return out.reshape(1, m, m)


def solution(mesh):
    n_j, n_p = mesh.shape["jown"], mesh.shape["pown"]
    cores = 2
    side = math.isqrt(n_p)
    dims = (n_j, n_p, n_j // cores, side, n_p // side, cores)
    placed = (
        P(("jown", "pown"), None, None),
        P(("jown", "pown"), None, None),
        P(("jown", "pown"), None),
        P(("jown", "pown"), None),
        P(),
        P(),
        P(None, None, ("jown", "pown")),
        P(),
        P(None, None, ("jown", "pown")),
    )
    return jax.shard_map(
        functools.partial(per_device, dims),
        mesh=mesh,
        in_specs=placed,
        out_specs=P(("jown", "pown"), None, None),
        check_vma=False,
    )
```

```python
import functools
import math

import jax
import jax.numpy as jnp
from jax import lax
from jax.experimental import pallas as pl
from jax.experimental.pallas import tpu as pltpu
from jax.sharding import PartitionSpec as P

MESH = pl.DeviceIdType.MESH
F32, BF16 = jnp.float32, jnp.bfloat16
STRIDE = 37
PARTS = (4, 4)
UNROLL = 2
VMEM_MIB = 42


def kernel(
    dims,
    orders_hbm,
    psrc_hbm,
    bsrc_hbm,
    bands_hbm,
    vertex_hbm,
    bare_hbm,
    pp_hbm,
    php_hbm,
    psix_hbm,
    bsix_hbm,
    out_ref,
    orders_ref,
    psrc_ref,
    bsrc_ref,
    pp_ref,
    php_ref,
    psix_ref,
    bsix_ref,
    vbuf,
    bbuf,
    base,
    wide,
    ph,
    weighted,
    load_sem,
    send_sem,
    recv_sem,
    gate_sem,
    peers,
    *tile_bufs,
):
    n_parts = len(PARTS)
    parts = range(n_parts)
    recv_a, mix_a, ph_bands, cyc, recv_b, mix_b, ret_bands = (
        tile_bufs[n_parts * i : n_parts * (i + 1)] for i in range(7)
    )
    starts = [sum(PARTS[:part]) for part in parts]
    n_j, n_p, n_y, n_x, n_z, cores = dims
    total = n_j * n_p
    m = ph.shape[0]
    band = m // total
    me_j, me_p = lax.axis_index("jown"), lax.axis_index("pown")
    me = me_j * n_p + me_p
    my_y, my_c = me_j // cores, me_j % cores
    my_x, my_z = me_p // n_z, me_p % n_z

    owners = [[(my_y + y) % n_y * cores + (my_c + c) % cores for c in range(cores)] for y in range(n_y)]
    places = [[(my_x + x) % n_x * n_z + (my_z + z) % n_z for z in range(n_z)] for x in range(n_x)]

    def shifted(y, c, x, z):
        return owners[y][c], places[x][z]

    def offset_of(step):
        o = (step * STRIDE) % total
        z = o % n_z
        o = o // n_z
        x = o % n_x
        o = o // n_x
        return o // cores, o % cores, x, z

    def peer_of(step):
        return peers[0, step], peers[1, step], peers[2, step]

    def send(src, dst, phase, part, j, p):
        pltpu.make_async_remote_copy(
            src_ref=src,
            dst_ref=dst,
            send_sem=send_sem.at[phase, part],
            recv_sem=recv_sem.at[phase, part],
            device_id=(j, p),
            device_id_type=MESH,
        ).start()

    def wait_all(part, sem):
        span = mix_a[part].at[pl.ds(0, total - 1)]
        pltpu.make_async_copy(span, span, sem).wait()

    def arrived(phase, part):
        wait_all(part, recv_sem.at[phase, part])

    def changed(offset):
        return sum(d != 0 for d in (offset[0], offset[2], offset[3]))

    offsets = [offset_of(step) for step in range(1, total)]
    rings = [
        [o for o in offsets if changed(o) <= 1],
        [o for o in offsets if changed(o) == 2],
        [o for o in offsets if changed(o) == 3],
    ]
    along = [o for o in rings[0] if o[1] == 0]
    barrier = pltpu.get_barrier_semaphore()
    for offset in rings[0]:
        pl.semaphore_signal(barrier, inc=1, device_id=shifted(*offset), device_id_type=MESH)

    for step in range(total):
        j, p = shifted(*offset_of(step))
        peers[0, step] = j
        peers[1, step] = p
        peers[2, step] = j * n_p + p

    def load(src, dst, slot):
        copy = pltpu.make_async_copy(src, dst, load_sem.at[slot])
        copy.start()
        return copy

    rows_of = [pl.ds(starts[part] * band, PARTS[part] * band) for part in parts]
    own = [load(bands_hbm.at[me, rows_of[part]], recv_a[part].at[me], 9 + part) for part in parts]
    loads = [
        load(src, dst, slot)
        for slot, (src, dst) in enumerate(
            (
                (orders_hbm, orders_ref),
                (psrc_hbm, psrc_ref),
                (bsrc_hbm, bsrc_ref),
                (pp_hbm, pp_ref),
                (php_hbm, php_ref),
                (psix_hbm, psix_ref),
                (bsix_hbm, bsix_ref),
                (vertex_hbm, vbuf),
                (bare_hbm, bbuf),
            )
        )
    ]

    def leave_raw(part, offset):
        j, p = shifted(*offset)
        send(bands_hbm.at[j * n_p + p, rows_of[part]], recv_a[part].at[me], 0, part, j, p)

    pl.semaphore_wait(barrier, len(rings[0]))
    for stage, ring in enumerate(rings):
        if stage < 2:
            for offset in along:
                pl.semaphore_signal(gate_sem.at[stage], inc=1, device_id=shifted(*offset), device_id_type=MESH)
        for offset in ring:
            leave_raw(0, offset)
        if stage < 2:
            pl.semaphore_wait(gate_sem.at[stage], len(along))
    for part in parts[1:]:
        for offset in offsets:
            leave_raw(part, offset)

    for copy in loads:
        copy.wait()
    my_order = orders_ref[me]
    lane = lax.broadcasted_iota(jnp.int32, (8, 128), 1)
    row_id = me * band + lax.broadcasted_iota(jnp.int32, (8, 128), 0)

    def spread(six_ref, slot):
        for k in range(4):
            six = six_ref[k]
            for c in range(total):
                wide[slot, c, k] = jnp.broadcast_to(six[:, c : c + 1], (8, 128))

    spread(psix_ref, 0)

    def recouple(recv, part, mix, landing, src_ref, slot, source_mask, phase):
        first, tiles = 128 * starts[part], PARTS[part]

        def mixed(c):
            order = orders_ref[c]
            acc = [None] * tiles
            for k in range(4):
                s = src_ref[k, c]
                bound = order
                if source_mask:
                    bound = jnp.minimum(order, orders_ref[s])
                w = jnp.where(row_id < bound, wide[slot, c, k], 0.0)
                x = recv[part][s].astype(F32)
                for t in range(tiles):
                    term = w * x[8 * t : 8 * t + 8]
                    if source_mask:
                        term = jnp.where(lane < bound - (first + 128 * t), term, 0.0)
                    acc[t] = term if k == 0 else acc[t] + term
            if not source_mask:
                acc = [jnp.where(lane < order - (first + 128 * t), a, 0.0) for t, a in enumerate(acc)]
            return jnp.concatenate(acc, axis=0).astype(BF16)

        def store(step):
            c = peer_of(step)[2]
            mix[part][c] = mixed(c)

        def leave(step):
            j, p, c = peer_of(step)
            send(mix[part].at[c], landing[part].at[me], phase, part, j, p)

        store(1)

        @pl.loop(2, total, unroll=UNROLL)
        def _(step):
            store(step)
            leave(step - 1)

        landing[part][me] = mixed(me)
        leave(total - 1)

    for part in parts:
        own[part].wait()
        arrived(0, part)
        recouple(recv_a, part, mix_a, ph_bands, psrc_ref, 0, True, 1)

    col_live = (lax.broadcasted_iota(jnp.int32, (1, m), 1) < my_order).astype(F32)

    @pl.loop(0, m // 128)
    def _(i):
        rows = pl.ds(pl.multiple_of(i * 128, 128), 128)
        ids = i * 128 + lax.broadcasted_iota(jnp.int32, (128, 1), 0)
        row_live = (ids < my_order).astype(F32)
        scale = jnp.broadcast_to(pp_ref[:, rows], (128, 128)).T
        masked = vbuf[rows, :].astype(F32) * col_live * row_live
        base[rows, :] = masked
        for t in range(m // 128):
            cols = slice(128 * t, 128 * t + 128)
            weighted[rows, cols] = (masked[:, cols] * scale).astype(BF16)

    @pl.loop(0, m // 256)
    def _(i):
        rows = pl.ds(pl.multiple_of(i * 256, 256), 256)
        base[rows, :] += jnp.dot(bbuf[rows, :], weighted[...], preferred_element_type=F32)

    spread(bsix_ref, 1)

    def pair(bands, one, two):
        a = bands[one].astype(F32)
        b = bands[two].astype(F32)
        return [
            jnp.concatenate([a[8 * t : 8 * t + 8], b[8 * t : 8 * t + 8]], axis=0)
            for t in range(bands.shape[1] // 8)
        ]

    for part in parts:
        arrived(1, part)

        @pl.loop(0, total // 2, unroll=UNROLL)
        def _(q):
            rows = pl.ds(pl.multiple_of(q * 16, 16), 16)
            for t, tile in enumerate(pair(ph_bands[part], 2 * q, 2 * q + 1)):
                ph[rows, 128 * (starts[part] + t) : 128 * (starts[part] + t) + 128] = tile.astype(BF16)
            for t, tile in enumerate(pair(ph_bands[part], peer_of(2 * q)[2], peer_of(2 * q + 1)[2])):
                cols = slice(128 * (starts[part] + t), 128 * (starts[part] + t) + 128)
                weighted[rows, cols] = (tile * php_ref[:, cols]).astype(BF16)

    per_chunk = 256 // band
    for part in parts:
        cols = slice(128 * starts[part], 128 * (starts[part] + PARTS[part]))

        @pl.loop(0, total // per_chunk)
        def _(i):
            rows = pl.ds(pl.multiple_of(i * 256, 256), 256)
            prod = jnp.dot(weighted[rows, :], ph[:, cols], preferred_element_type=F32)
            prod = prod * (1.0 / math.sqrt(m))
            for b in range(per_chunk):
                lines = [prod[band * b : band * b + band, 128 * t : 128 * t + 128] for t in range(PARTS[part])]
                cyc[part][i * per_chunk + b] = jnp.concatenate(lines, axis=0).astype(BF16)

            @pl.loop(0, per_chunk)
            def _(b):
                step = i * per_chunk + b

                @pl.when(step > 0)
                def _():
                    j, p, _ = peer_of(step)
                    send(cyc[part].at[step], recv_b[part].at[me], 2, part, j, p)

        recv_b[part][me] = cyc[part][0]

    for part in parts:
        arrived(2, part)
        recouple(recv_b, part, mix_b, ret_bands, bsrc_ref, 1, False, 3)

    for part in parts:
        arrived(3, part)

        @pl.loop(0, total // 2, unroll=UNROLL)
        def _(q):
            rows = pl.ds(pl.multiple_of(q * 16, 16), 16)
            ids = q * 16 + lax.broadcasted_iota(jnp.int32, (16, 128), 0)
            for t, tile in enumerate(pair(ret_bands[part], 2 * q, 2 * q + 1)):
                first = 128 * (starts[part] + t)
                cols = slice(first, first + 128)
                col_ids = first + lax.broadcasted_iota(jnp.int32, (16, 128), 1)
                keep = (ids < my_order) & (col_ids < my_order)
                out_ref[rows, cols] = jnp.where(keep, base[rows, cols] + tile, 0.0).astype(BF16)

    for phase in range(4):
        for part in parts:
            wait_all(part, send_sem.at[phase, part])


def per_device(dims, vertex, bare, pp_prop, ph_prop, orders, pandya_src, pandya_sixj, back_src, back_sixj):
    m = vertex.shape[1]
    n_j, n_p = dims[:2]
    total = n_j * n_p
    band = m // total
    tiles = m // 128
    flat = vertex.reshape(m, m)
    bands = flat.reshape(total, band, tiles, 128).transpose(0, 2, 1, 3).reshape(total, tiles * band, 128)
    part_bufs = [pltpu.VMEM((total, band * part, 128), BF16) for part in PARTS]
    square = pltpu.VMEM((m, m), BF16)
    vmem = pl.BlockSpec(memory_space=pltpu.VMEM)
    hbm = pl.BlockSpec(memory_space=pltpu.HBM)
    out = pl.pallas_call(
        functools.partial(kernel, dims),
        out_shape=jax.ShapeDtypeStruct((m, m), BF16),
        in_specs=[hbm] * 10,
        out_specs=vmem,
        scratch_shapes=[
            pltpu.SMEM((total,), jnp.int32),
            pltpu.SMEM((4, total), jnp.int32),
            pltpu.SMEM((4, total), jnp.int32),
            pltpu.VMEM((1, m), F32),
            pltpu.VMEM((1, m), F32),
            pltpu.VMEM((4, band, total), F32),
            pltpu.VMEM((4, band, total), F32),
            square,
            square,
            pltpu.VMEM((m, m), F32),
            pltpu.VMEM((2, total, 4, 8, 128), F32),
            square,
            square,
            pltpu.SemaphoreType.DMA((9 + len(PARTS),)),
            pltpu.SemaphoreType.DMA((4, len(PARTS))),
            pltpu.SemaphoreType.DMA((4, len(PARTS))),
            pltpu.SemaphoreType.REGULAR((2,)),
            pltpu.SMEM((3, total), jnp.int32),
        ]
        + part_bufs * 7,
        compiler_params=pltpu.CompilerParams(collective_id=0, has_side_effects=True, vmem_limit_bytes=VMEM_MIB * 1024 * 1024),
        name="parquet",
    )(
        *(pltpu.with_memory_space_constraint(a, pltpu.HBM) for a in (
        orders,
        pandya_src.T,
        back_src.T,
        bands,
        flat,
        bare.reshape(m, m),
        pp_prop,
        ph_prop,
        pandya_sixj.transpose(1, 2, 0),
        back_sixj.transpose(1, 2, 0),
    )))
    return out.reshape(1, m, m)


def solution(mesh):
    n_j, n_p = mesh.shape["jown"], mesh.shape["pown"]
    cores = 2
    side = math.isqrt(n_p)
    dims = (n_j, n_p, n_j // cores, side, n_p // side, cores)
    placed = (
        P(("jown", "pown"), None, None),
        P(("jown", "pown"), None, None),
        P(("jown", "pown"), None),
        P(("jown", "pown"), None),
        P(),
        P(),
        P(None, None, ("jown", "pown")),
        P(),
        P(None, None, ("jown", "pown")),
    )
    return jax.shard_map(
        functools.partial(per_device, dims),
        mesh=mesh,
        in_specs=placed,
        out_specs=P(("jown", "pown"), None, None),
        check_vma=False,
    )
```

```python
import functools
import math

import jax
import jax.numpy as jnp
from jax import lax
from jax.experimental import pallas as pl
from jax.experimental.pallas import tpu as pltpu
from jax.sharding import PartitionSpec as P

MESH = pl.DeviceIdType.MESH
F32, BF16 = jnp.float32, jnp.bfloat16
STRIDE = 37
PARTS = (6, 2)
UNROLL = 4
CHUNK = 256
VMEM_MIB = 44


def kernel(
    dims,
    orders_hbm,
    psrc_hbm,
    bsrc_hbm,
    bands_hbm,
    vertex_hbm,
    bare_hbm,
    pp_hbm,
    php_hbm,
    psix_hbm,
    bsix_hbm,
    out_ref,
    orders_ref,
    psrc_ref,
    bsrc_ref,
    pp_ref,
    php_ref,
    psix_ref,
    bsix_ref,
    vbuf,
    bbuf,
    base,
    wide,
    ph,
    weighted,
    load_sem,
    send_sem,
    recv_sem,
    gate_sem,
    peers,
    early,
    *tile_bufs,
):
    n_parts = len(PARTS)
    parts = range(n_parts)
    recv_a, mix_a, ph_bands, cyc, recv_b, mix_b, ret_bands = (
        tile_bufs[n_parts * i : n_parts * (i + 1)] for i in range(7)
    )
    starts = [sum(PARTS[:part]) for part in parts]
    n_j, n_p, n_y, n_x, n_z, cores = dims
    total = n_j * n_p
    m = ph.shape[0]
    band = m // total
    me_j, me_p = lax.axis_index("jown"), lax.axis_index("pown")
    me = me_j * n_p + me_p
    my_y, my_c = me_j // cores, me_j % cores
    my_x, my_z = me_p // n_z, me_p % n_z

    owners = [[(my_y + y) % n_y * cores + (my_c + c) % cores for c in range(cores)] for y in range(n_y)]
    places = [[(my_x + x) % n_x * n_z + (my_z + z) % n_z for z in range(n_z)] for x in range(n_x)]

    def shifted(y, c, x, z):
        return owners[y][c], places[x][z]

    def offset_of(step):
        o = (step * STRIDE) % total
        z = o % n_z
        o = o // n_z
        x = o % n_x
        o = o // n_x
        return o // cores, o % cores, x, z

    def peer_of(step):
        return peers[0, step], peers[1, step], peers[2, step]

    def send(src, dst, phase, part, j, p):
        pltpu.make_async_remote_copy(
            src_ref=src,
            dst_ref=dst,
            send_sem=send_sem.at[phase, part],
            recv_sem=recv_sem.at[phase, part],
            device_id=(j, p),
            device_id_type=MESH,
        ).start()

    def wait_all(part, sem):
        span = mix_a[part].at[pl.ds(0, total - 1)]
        pltpu.make_async_copy(span, span, sem).wait()

    def arrived(phase, part):
        wait_all(part, recv_sem.at[phase, part])

    def changed(offset):
        return sum(d != 0 for d in (offset[0], offset[2], offset[3]))

    offsets = [offset_of(step) for step in range(1, total)]
    rings = [
        [o for o in offsets if changed(o) <= 1],
        [o for o in offsets if changed(o) == 2],
        [o for o in offsets if changed(o) == 3],
    ]
    along = [o for o in rings[0] if o[1] == 0]
    barrier = pltpu.get_barrier_semaphore()
    for offset in rings[0]:
        pl.semaphore_signal(barrier, inc=1, device_id=shifted(*offset), device_id_type=MESH)

    def load(src, dst, slot):
        copy = pltpu.make_async_copy(src, dst, load_sem.at[slot])
        copy.start()
        return copy

    rows_of = [pl.ds(starts[part] * band, PARTS[part] * band) for part in parts]
    own = [load(bands_hbm.at[me, rows_of[part]], recv_a[part].at[me], 9 + part) for part in parts]
    loads = [
        load(src, dst, slot)
        for slot, (src, dst) in enumerate(
            (
                (orders_hbm, orders_ref),
                (psrc_hbm, psrc_ref),
                (bsrc_hbm, bsrc_ref),
                (pp_hbm, pp_ref),
                (php_hbm, php_ref),
                (psix_hbm, psix_ref),
                (bsix_hbm, bsix_ref),
                (vertex_hbm, vbuf),
                (bare_hbm, bbuf),
            )
        )
    ]

    def leave_raw(part, offset):
        j, p = shifted(*offset)
        send(bands_hbm.at[j * n_p + p, rows_of[part]], recv_a[part].at[me], 0, part, j, p)

    pl.semaphore_wait(barrier, len(rings[0]))
    for stage, ring in enumerate(rings):
        if stage < 2:
            for offset in along:
                pl.semaphore_signal(gate_sem.at[stage], inc=1, device_id=shifted(*offset), device_id_type=MESH)
        for offset in ring:
            leave_raw(0, offset)
        if stage < 2:
            pl.semaphore_wait(gate_sem.at[stage], len(along))
    for part in parts[1:]:
        for offset in offsets:
            leave_raw(part, offset)

    for step in range(total):
        j, p = shifted(*offset_of(step))
        peers[0, step] = j
        peers[1, step] = p
        peers[2, step] = j * n_p + p

    for copy in loads:
        copy.wait()
    my_order = orders_ref[me]
    lane = lax.broadcasted_iota(jnp.int32, (8, 128), 1)
    row_id = me * band + lax.broadcasted_iota(jnp.int32, (8, 128), 0)

    def spread(six_ref, slot):
        for k in range(4):
            six = six_ref[k]
            for c in range(total):
                wide[slot, c, k] = jnp.broadcast_to(six[:, c : c + 1], (8, 128))

    spread(psix_ref, 0)

    def recouple(recv, part, mix, landing, src_ref, slot, source_mask, phase):
        first, tiles = 128 * starts[part], PARTS[part]

        def mixed(c):
            order = orders_ref[c]
            acc = [None] * tiles
            for k in range(4):
                s = src_ref[k, c]
                bound = order
                if source_mask:
                    bound = jnp.minimum(order, orders_ref[s])
                w = jnp.where(row_id < bound, wide[slot, c, k], 0.0)
                x = recv[part][s].astype(F32)
                for t in range(tiles):
                    term = w * x[8 * t : 8 * t + 8]
                    if source_mask:
                        term = jnp.where(lane < bound - (first + 128 * t), term, 0.0)
                    acc[t] = term if k == 0 else acc[t] + term
            if not source_mask:
                acc = [jnp.where(lane < order - (first + 128 * t), a, 0.0) for t, a in enumerate(acc)]
            return jnp.concatenate(acc, axis=0).astype(BF16)

        def store(step):
            c = peer_of(step)[2]
            mix[part][c] = mixed(c)

        def leave(step):
            j, p, c = peer_of(step)
            send(mix[part].at[c], landing[part].at[me], phase, part, j, p)

        store(1)

        @pl.loop(2, total, unroll=UNROLL)
        def _(step):
            store(step)
            leave(step - 1)

        landing[part][me] = mixed(me)
        leave(total - 1)

    for part in parts:
        own[part].wait()
        arrived(0, part)
        recouple(recv_a, part, mix_a, ph_bands, psrc_ref, 0, True, 1)

    col_live = (lax.broadcasted_iota(jnp.int32, (1, m), 1) < my_order).astype(F32)

    @pl.loop(0, m // 128)
    def _(i):
        rows = pl.ds(pl.multiple_of(i * 128, 128), 128)
        ids = i * 128 + lax.broadcasted_iota(jnp.int32, (128, 1), 0)
        row_live = (ids < my_order).astype(F32)
        scale = jnp.broadcast_to(pp_ref[:, rows], (128, 128)).T
        masked = vbuf[rows, :].astype(F32) * col_live * row_live
        base[rows, :] = masked
        for t in range(m // 128):
            cols = slice(128 * t, 128 * t + 128)
            weighted[rows, cols] = (masked[:, cols] * scale).astype(BF16)

    @pl.loop(0, m // 256)
    def _(i):
        rows = pl.ds(pl.multiple_of(i * 256, 256), 256)
        base[rows, :] += jnp.dot(bbuf[rows, :], weighted[...], preferred_element_type=F32)

    spread(bsix_ref, 1)

    def pair(bands, one, two):
        a = bands[one].astype(F32)
        b = bands[two].astype(F32)
        return [
            jnp.concatenate([a[8 * t : 8 * t + 8], b[8 * t : 8 * t + 8]], axis=0)
            for t in range(bands.shape[1] // 8)
        ]

    def columns(part):
        return slice(128 * starts[part], 128 * (starts[part] + PARTS[part]))

    def place_ph(part):
        @pl.loop(0, total // 2, unroll=UNROLL)
        def _(q):
            rows = pl.ds(pl.multiple_of(q * 16, 16), 16)
            for t, tile in enumerate(pair(ph_bands[part], 2 * q, 2 * q + 1)):
                ph[rows, 128 * (starts[part] + t) : 128 * (starts[part] + t) + 128] = tile.astype(BF16)

    def place_weighted(part, first, count):
        @pl.loop(0, count, unroll=UNROLL)
        def _(at):
            q = first + at
            rows = pl.ds(pl.multiple_of(q * 16, 16), 16)
            for t, tile in enumerate(pair(ph_bands[part], peer_of(2 * q)[2], peer_of(2 * q + 1)[2])):
                cols = slice(128 * (starts[part] + t), 128 * (starts[part] + t) + 128)
                weighted[rows, cols] = (tile * php_ref[:, cols]).astype(BF16)

    per_chunk = CHUNK // band

    def leave_product(part, i, prod):
        prod = prod * (1.0 / math.sqrt(m))
        for b in range(per_chunk):
            lines = [prod[band * b : band * b + band, 128 * t : 128 * t + 128] for t in range(PARTS[part])]
            cyc[part][i * per_chunk + b] = jnp.concatenate(lines, axis=0).astype(BF16)

        @pl.loop(0, per_chunk)
        def _(b):
            step = i * per_chunk + b

            @pl.when(step > 0)
            def _():
                j, p, _ = peer_of(step)
                send(cyc[part].at[step], recv_b[part].at[me], 2, part, j, p)

    left, right = columns(0), columns(1)
    arrived(1, 0)
    place_ph(0)
    place_weighted(0, 0, total // 2)

    @pl.loop(0, m // CHUNK)
    def _(i):
        rows = pl.ds(pl.multiple_of(i * CHUNK, CHUNK), CHUNK)
        early[rows, :] = jnp.dot(weighted[rows, left], ph[left, left], preferred_element_type=F32)

    arrived(1, 1)

    @pl.loop(0, m // CHUNK)
    def _(i):
        rows = pl.ds(pl.multiple_of(i * CHUNK, CHUNK), CHUNK)
        place_weighted(1, i * (per_chunk // 2), per_chunk // 2)
        late = jnp.dot(weighted[rows, right], ph[right, left], preferred_element_type=F32)
        leave_product(0, i, early[rows, :] + late)

    place_ph(1)

    @pl.loop(0, m // CHUNK)
    def _(i):
        rows = pl.ds(pl.multiple_of(i * CHUNK, CHUNK), CHUNK)
        leave_product(1, i, jnp.dot(weighted[rows, :], ph[:, right], preferred_element_type=F32))

    for part in parts:
        recv_b[part][me] = cyc[part][0]

    for part in parts:
        arrived(2, part)
        recouple(recv_b, part, mix_b, ret_bands, bsrc_ref, 1, False, 3)

    for part in parts:
        arrived(3, part)

        @pl.loop(0, total // 2, unroll=UNROLL)
        def _(q):
            rows = pl.ds(pl.multiple_of(q * 16, 16), 16)
            ids = q * 16 + lax.broadcasted_iota(jnp.int32, (16, 128), 0)
            for t, tile in enumerate(pair(ret_bands[part], 2 * q, 2 * q + 1)):
                first = 128 * (starts[part] + t)
                cols = slice(first, first + 128)
                col_ids = first + lax.broadcasted_iota(jnp.int32, (16, 128), 1)
                keep = (ids < my_order) & (col_ids < my_order)
                out_ref[rows, cols] = jnp.where(keep, base[rows, cols] + tile, 0.0).astype(BF16)

    for phase in range(4):
        for part in parts:
            wait_all(part, send_sem.at[phase, part])


def per_device(dims, vertex, bare, pp_prop, ph_prop, orders, pandya_src, pandya_sixj, back_src, back_sixj):
    m = vertex.shape[1]
    n_j, n_p = dims[:2]
    total = n_j * n_p
    band = m // total
    tiles = m // 128
    flat = vertex.reshape(m, m)
    bands = flat.reshape(total, band, tiles, 128).transpose(0, 2, 1, 3).reshape(total, tiles * band, 128)
    part_bufs = [pltpu.VMEM((total, band * part, 128), BF16) for part in PARTS]
    square = pltpu.VMEM((m, m), BF16)
    vmem = pl.BlockSpec(memory_space=pltpu.VMEM)
    hbm = pl.BlockSpec(memory_space=pltpu.HBM)
    out = pl.pallas_call(
        functools.partial(kernel, dims),
        out_shape=jax.ShapeDtypeStruct((m, m), BF16),
        in_specs=[hbm] * 10,
        out_specs=vmem,
        scratch_shapes=[
            pltpu.SMEM((total,), jnp.int32),
            pltpu.SMEM((4, total), jnp.int32),
            pltpu.SMEM((4, total), jnp.int32),
            pltpu.VMEM((1, m), F32),
            pltpu.VMEM((1, m), F32),
            pltpu.VMEM((4, band, total), F32),
            pltpu.VMEM((4, band, total), F32),
            square,
            square,
            pltpu.VMEM((m, m), F32),
            pltpu.VMEM((2, total, 4, 8, 128), F32),
            square,
            square,
            pltpu.SemaphoreType.DMA((9 + len(PARTS),)),
            pltpu.SemaphoreType.DMA((4, len(PARTS))),
            pltpu.SemaphoreType.DMA((4, len(PARTS))),
            pltpu.SemaphoreType.REGULAR((2,)),
            pltpu.SMEM((3, total), jnp.int32),
            pltpu.VMEM((m, 128 * PARTS[0]), F32),
        ]
        + part_bufs * 7,
        compiler_params=pltpu.CompilerParams(collective_id=0, has_side_effects=True, vmem_limit_bytes=VMEM_MIB * 1024 * 1024),
        name="parquet",
    )(
        *(pltpu.with_memory_space_constraint(a, pltpu.HBM) for a in (
        orders,
        pandya_src.T,
        back_src.T,
        bands,
        flat,
        bare.reshape(m, m),
        pp_prop,
        ph_prop,
        pandya_sixj.transpose(1, 2, 0),
        back_sixj.transpose(1, 2, 0),
    )))
    return out.reshape(1, m, m)


def solution(mesh):
    n_j, n_p = mesh.shape["jown"], mesh.shape["pown"]
    cores = 2
    side = math.isqrt(n_p)
    dims = (n_j, n_p, n_j // cores, side, n_p // side, cores)
    placed = (
        P(("jown", "pown"), None, None),
        P(("jown", "pown"), None, None),
        P(("jown", "pown"), None),
        P(("jown", "pown"), None),
        P(),
        P(),
        P(None, None, ("jown", "pown")),
        P(),
        P(None, None, ("jown", "pown")),
    )
    return jax.shard_map(
        functools.partial(per_device, dims),
        mesh=mesh,
        in_specs=placed,
        out_specs=P(("jown", "pown"), None, None),
        check_vma=False,
    )
```

```python
import functools
import math

import jax
import jax.numpy as jnp
from jax import lax
from jax.experimental import pallas as pl
from jax.experimental.pallas import tpu as pltpu
from jax.sharding import PartitionSpec as P

MESH = pl.DeviceIdType.MESH
F32, BF16 = jnp.float32, jnp.bfloat16
STRIDE = 45
PARTS = (6, 2)
UNROLL = 4
CHUNK = 256
VMEM_MIB = 47


def kernel(
    dims,
    orders_hbm,
    psrc_hbm,
    bsrc_hbm,
    bands_hbm,
    vertex_hbm,
    bare_hbm,
    pp_hbm,
    php_hbm,
    psix_hbm,
    bsix_hbm,
    out_ref,
    orders_ref,
    psrc_ref,
    bsrc_ref,
    pp_ref,
    php_ref,
    psix_ref,
    bsix_ref,
    vbuf,
    bbuf,
    base,
    wide,
    ph,
    weighted,
    load_sem,
    send_sem,
    recv_sem,
    gate_sem,
    peers,
    early,
    bands,
    *tile_bufs,
):
    n_parts = len(PARTS)
    parts = range(n_parts)
    recv_a, mix_a, ph_bands, cyc, recv_b, mix_b, ret_bands = (
        tile_bufs[n_parts * i : n_parts * (i + 1)] for i in range(7)
    )
    starts = [sum(PARTS[:part]) for part in parts]
    n_j, n_p, n_y, n_x, n_z, cores = dims
    total = n_j * n_p
    m = ph.shape[0]
    band = m // total
    me_j, me_p = lax.axis_index("jown"), lax.axis_index("pown")
    me = me_j * n_p + me_p
    my_y, my_c = me_j // cores, me_j % cores
    my_x, my_z = me_p // n_z, me_p % n_z

    owners = [[(my_y + y) % n_y * cores + (my_c + c) % cores for c in range(cores)] for y in range(n_y)]
    places = [[(my_x + x) % n_x * n_z + (my_z + z) % n_z for z in range(n_z)] for x in range(n_x)]

    def shifted(y, c, x, z):
        return owners[y][c], places[x][z]

    def offset_of(step):
        o = (step * STRIDE) % total
        z = o % n_z
        o = o // n_z
        x = o % n_x
        o = o // n_x
        return o // cores, o % cores, x, z

    def peer_of(step):
        return peers[0, step], peers[1, step], peers[2, step]

    def send(src, dst, phase, part, j, p):
        pltpu.make_async_remote_copy(
            src_ref=src,
            dst_ref=dst,
            send_sem=send_sem.at[phase, part],
            recv_sem=recv_sem.at[phase, part],
            device_id=(j, p),
            device_id_type=MESH,
        ).start()

    def wait_all(part, sem):
        span = mix_a[part].at[pl.ds(0, total - 1)]
        pltpu.make_async_copy(span, span, sem).wait()

    def arrived(phase, part):
        wait_all(part, recv_sem.at[phase, part])

    def changed(offset):
        return sum(d != 0 for d in (offset[0], offset[2], offset[3]))

    offsets = [offset_of(step) for step in range(1, total)]
    rings = [
        [o for o in offsets if changed(o) <= 1],
        [o for o in offsets if changed(o) == 2],
        [o for o in offsets if changed(o) == 3],
    ]
    along = [o for o in rings[0] if o[1] == 0]
    barrier = pltpu.get_barrier_semaphore()
    for offset in rings[0]:
        pl.semaphore_signal(barrier, inc=1, device_id=shifted(*offset), device_id_type=MESH)

    def load(src, dst, slot):
        copy = pltpu.make_async_copy(src, dst, load_sem.at[slot])
        copy.start()
        return copy

    raw = load(bands_hbm, bands, 9 + n_parts)
    rows_of = [pl.ds(starts[part] * band, PARTS[part] * band) for part in parts]
    own = [load(bands_hbm.at[me, rows_of[part]], recv_a[part].at[me], 9 + part) for part in parts]
    loads = [
        load(src, dst, slot)
        for slot, (src, dst) in enumerate(
            (
                (orders_hbm, orders_ref),
                (psrc_hbm, psrc_ref),
                (bsrc_hbm, bsrc_ref),
                (pp_hbm, pp_ref),
                (php_hbm, php_ref),
                (psix_hbm, psix_ref),
                (bsix_hbm, bsix_ref),
                (vertex_hbm, vbuf),
                (bare_hbm, bbuf),
            )
        )
    ]

    def leave_raw(part, offset):
        j, p = shifted(*offset)
        send(bands.at[j * n_p + p, rows_of[part]], recv_a[part].at[me], 0, part, j, p)

    pl.semaphore_wait(barrier, len(rings[0]))
    raw.wait()
    for stage, ring in enumerate(rings):
        if stage < 2:
            for offset in along:
                pl.semaphore_signal(gate_sem.at[stage], inc=1, device_id=shifted(*offset), device_id_type=MESH)
        for part in parts if stage == 0 else (0,):
            for offset in ring:
                leave_raw(part, offset)
        if stage < 2:
            pl.semaphore_wait(gate_sem.at[stage], len(along))
    for part in parts[1:]:
        for offset in offsets:
            if offset not in rings[0]:
                leave_raw(part, offset)

    for step in range(total):
        j, p = shifted(*offset_of(step))
        peers[0, step] = j
        peers[1, step] = p
        peers[2, step] = j * n_p + p

    for copy in loads:
        copy.wait()
    my_order = orders_ref[me]
    lane = lax.broadcasted_iota(jnp.int32, (8, 128), 1)
    row_id = me * band + lax.broadcasted_iota(jnp.int32, (8, 128), 0)

    def spread(six_ref, slot):
        for k in range(4):
            six = six_ref[k]
            for c in range(total):
                wide[slot, c, k] = jnp.broadcast_to(six[:, c : c + 1], (8, 128))

    spread(psix_ref, 0)

    def recouple(recv, part, mix, landing, src_ref, slot, source_mask, phase):
        first, tiles = 128 * starts[part], PARTS[part]

        def mixed(c):
            order = orders_ref[c]
            acc = [None] * tiles
            for k in range(4):
                s = src_ref[k, c]
                bound = order
                if source_mask:
                    bound = jnp.minimum(order, orders_ref[s])
                w = jnp.where(row_id < bound, wide[slot, c, k], 0.0)
                x = recv[part][s].astype(F32)
                for t in range(tiles):
                    term = w * x[8 * t : 8 * t + 8]
                    if source_mask:
                        term = jnp.where(lane < bound - (first + 128 * t), term, 0.0)
                    acc[t] = term if k == 0 else acc[t] + term
            if not source_mask:
                acc = [jnp.where(lane < order - (first + 128 * t), a, 0.0) for t, a in enumerate(acc)]
            return jnp.concatenate(acc, axis=0).astype(BF16)

        def store(step):
            c = peer_of(step)[2]
            mix[part][c] = mixed(c)

        def leave(step):
            j, p, c = peer_of(step)
            send(mix[part].at[c], landing[part].at[me], phase, part, j, p)

        store(1)

        @pl.loop(2, total, unroll=UNROLL)
        def _(step):
            store(step)
            leave(step - 1)

        landing[part][me] = mixed(me)
        leave(total - 1)

    for part in parts:
        own[part].wait()
        arrived(0, part)
        recouple(recv_a, part, mix_a, ph_bands, psrc_ref, 0, True, 1)

    col_live = (lax.broadcasted_iota(jnp.int32, (1, m), 1) < my_order).astype(F32)

    @pl.loop(0, m // 128)
    def _(i):
        rows = pl.ds(pl.multiple_of(i * 128, 128), 128)
        ids = i * 128 + lax.broadcasted_iota(jnp.int32, (128, 1), 0)
        row_live = (ids < my_order).astype(F32)
        scale = jnp.broadcast_to(pp_ref[:, rows], (128, 128)).T
        masked = vbuf[rows, :].astype(F32) * col_live * row_live
        base[rows, :] = masked
        for t in range(m // 128):
            cols = slice(128 * t, 128 * t + 128)
            weighted[rows, cols] = (masked[:, cols] * scale).astype(BF16)

    @pl.loop(0, m // 256)
    def _(i):
        rows = pl.ds(pl.multiple_of(i * 256, 256), 256)
        base[rows, :] += jnp.dot(bbuf[rows, :], weighted[...], preferred_element_type=F32)

    spread(bsix_ref, 1)

    def pair(bands, one, two):
        a = bands[one].astype(F32)
        b = bands[two].astype(F32)
        return [
            jnp.concatenate([a[8 * t : 8 * t + 8], b[8 * t : 8 * t + 8]], axis=0)
            for t in range(bands.shape[1] // 8)
        ]

    def columns(part):
        return slice(128 * starts[part], 128 * (starts[part] + PARTS[part]))

    def place_ph(part):
        @pl.loop(0, total // 2, unroll=UNROLL)
        def _(q):
            rows = pl.ds(pl.multiple_of(q * 16, 16), 16)
            for t, tile in enumerate(pair(ph_bands[part], 2 * q, 2 * q + 1)):
                ph[rows, 128 * (starts[part] + t) : 128 * (starts[part] + t) + 128] = tile.astype(BF16)

    def place_weighted(part, first, count):
        @pl.loop(0, count, unroll=UNROLL)
        def _(at):
            q = first + at
            rows = pl.ds(pl.multiple_of(q * 16, 16), 16)
            for t, tile in enumerate(pair(ph_bands[part], peer_of(2 * q)[2], peer_of(2 * q + 1)[2])):
                cols = slice(128 * (starts[part] + t), 128 * (starts[part] + t) + 128)
                weighted[rows, cols] = (tile * php_ref[:, cols]).astype(BF16)

    per_chunk = CHUNK // band

    def leave_product(part, i, prod):
        prod = prod * (1.0 / math.sqrt(m))
        for b in range(per_chunk):
            lines = [prod[band * b : band * b + band, 128 * t : 128 * t + 128] for t in range(PARTS[part])]
            cyc[part][i * per_chunk + b] = jnp.concatenate(lines, axis=0).astype(BF16)

        @pl.loop(0, per_chunk)
        def _(b):
            step = i * per_chunk + b

            @pl.when(step > 0)
            def _():
                j, p, _ = peer_of(step)
                send(cyc[part].at[step], recv_b[part].at[me], 2, part, j, p)

    left, right = columns(0), columns(1)
    arrived(1, 0)
    place_ph(0)
    place_weighted(0, 0, total // 2)

    @pl.loop(0, m // CHUNK)
    def _(i):
        rows = pl.ds(pl.multiple_of(i * CHUNK, CHUNK), CHUNK)
        early[rows, :] = jnp.dot(weighted[rows, left], ph[left, left], preferred_element_type=F32)

    arrived(1, 1)

    @pl.loop(0, m // CHUNK)
    def _(i):
        rows = pl.ds(pl.multiple_of(i * CHUNK, CHUNK), CHUNK)
        place_weighted(1, i * (per_chunk // 2), per_chunk // 2)
        late = jnp.dot(weighted[rows, right], ph[right, left], preferred_element_type=F32)
        leave_product(0, i, early[rows, :] + late)

    place_ph(1)

    @pl.loop(0, m // CHUNK)
    def _(i):
        rows = pl.ds(pl.multiple_of(i * CHUNK, CHUNK), CHUNK)
        leave_product(1, i, jnp.dot(weighted[rows, :], ph[:, right], preferred_element_type=F32))

    for part in parts:
        recv_b[part][me] = cyc[part][0]

    for part in parts:
        arrived(2, part)
        recouple(recv_b, part, mix_b, ret_bands, bsrc_ref, 1, False, 3)

    for part in parts:
        arrived(3, part)

        @pl.loop(0, total // 2, unroll=UNROLL)
        def _(q):
            rows = pl.ds(pl.multiple_of(q * 16, 16), 16)
            ids = q * 16 + lax.broadcasted_iota(jnp.int32, (16, 128), 0)
            for t, tile in enumerate(pair(ret_bands[part], 2 * q, 2 * q + 1)):
                first = 128 * (starts[part] + t)
                cols = slice(first, first + 128)
                col_ids = first + lax.broadcasted_iota(jnp.int32, (16, 128), 1)
                keep = (ids < my_order) & (col_ids < my_order)
                out_ref[rows, cols] = jnp.where(keep, base[rows, cols] + tile, 0.0).astype(BF16)

    for phase in range(4):
        for part in parts:
            wait_all(part, send_sem.at[phase, part])


def per_device(dims, vertex, bare, pp_prop, ph_prop, orders, pandya_src, pandya_sixj, back_src, back_sixj):
    m = vertex.shape[1]
    n_j, n_p = dims[:2]
    total = n_j * n_p
    band = m // total
    tiles = m // 128
    flat = vertex.reshape(m, m)
    bands = flat.reshape(total, band, tiles, 128).transpose(0, 2, 1, 3).reshape(total, tiles * band, 128)
    part_bufs = [pltpu.VMEM((total, band * part, 128), BF16) for part in PARTS]
    square = pltpu.VMEM((m, m), BF16)
    vmem = pl.BlockSpec(memory_space=pltpu.VMEM)
    hbm = pl.BlockSpec(memory_space=pltpu.HBM)
    out = pl.pallas_call(
        functools.partial(kernel, dims),
        out_shape=jax.ShapeDtypeStruct((m, m), BF16),
        in_specs=[hbm] * 10,
        out_specs=vmem,
        scratch_shapes=[
            pltpu.SMEM((total,), jnp.int32),
            pltpu.SMEM((4, total), jnp.int32),
            pltpu.SMEM((4, total), jnp.int32),
            pltpu.VMEM((1, m), F32),
            pltpu.VMEM((1, m), F32),
            pltpu.VMEM((4, band, total), F32),
            pltpu.VMEM((4, band, total), F32),
            square,
            square,
            pltpu.VMEM((m, m), F32),
            pltpu.VMEM((2, total, 4, 8, 128), F32),
            square,
            square,
            pltpu.SemaphoreType.DMA((10 + len(PARTS),)),
            pltpu.SemaphoreType.DMA((4, len(PARTS))),
            pltpu.SemaphoreType.DMA((4, len(PARTS))),
            pltpu.SemaphoreType.REGULAR((2,)),
            pltpu.SMEM((3, total), jnp.int32),
            pltpu.VMEM((m, 128 * PARTS[0]), F32),
            pltpu.VMEM((total, m * band // 128, 128), BF16),
        ]
        + part_bufs * 7,
        compiler_params=pltpu.CompilerParams(collective_id=0, has_side_effects=True, vmem_limit_bytes=VMEM_MIB * 1024 * 1024),
        name="parquet",
    )(
        *(pltpu.with_memory_space_constraint(a, pltpu.HBM) for a in (
        orders,
        pandya_src.T,
        back_src.T,
        bands,
        flat,
        bare.reshape(m, m),
        pp_prop,
        ph_prop,
        pandya_sixj.transpose(1, 2, 0),
        back_sixj.transpose(1, 2, 0),
    )))
    return out.reshape(1, m, m)


def solution(mesh):
    n_j, n_p = mesh.shape["jown"], mesh.shape["pown"]
    cores = 2
    side = math.isqrt(n_p)
    dims = (n_j, n_p, n_j // cores, side, n_p // side, cores)
    placed = (
        P(("jown", "pown"), None, None),
        P(("jown", "pown"), None, None),
        P(("jown", "pown"), None),
        P(("jown", "pown"), None),
        P(),
        P(),
        P(None, None, ("jown", "pown")),
        P(),
        P(None, None, ("jown", "pown")),
    )
    return jax.shard_map(
        functools.partial(per_device, dims),
        mesh=mesh,
        in_specs=placed,
        out_specs=P(("jown", "pown"), None, None),
        check_vma=False,
    )
```
